16 devices in a mesh: dp: 2 (over y, z), sp: 8 (over x, core).
Axes of the slice: x: 4, y: 2, z: 1, core: 2. Of those that a mesh axis runs over, the one named last changes fastest.
The devices are a block of a 4x4x8 slice.
Arguments:
- images: float32 [12, 448, 448, 3], P('dp', 'sp'), parts along dimension 0
- w_patch: bfloat16 [14, 14, 3, 1152], replicated
- b_patch: float32 [1152], replicated
- pos_embed: bfloat16 [1024, 1152], P('sp')
- ln1_gain: float32 [1152], replicated
- ln1_bias: float32 [1152], replicated
- w_qkv: bfloat16 [1152, 3, 16, 72], replicated
- b_qkv: float32 [3, 16, 72], replicated
- w_out: bfloat16 [16, 72, 1152], replicated
- b_out: float32 [1152], replicated
- ln2_gain: float32 [1152], replicated
- ln2_bias: float32 [1152], replicated
- w_fc1: bfloat16 [1152, 4304], replicated
- b_fc1: float32 [4304], replicated
- w_fc2: bfloat16 [4304, 1152], replicated
- b_fc2: float32 [1152], replicated
Outputs:
- output: bfloat16 [12, 1024, 1152], P('dp', 'sp'), parts along dimension 0
There are 2 independent parts. The reference program is written for one: setup_inputs(seed, part) draws one part's arguments, and reference() takes and returns one part's arrays. A program takes and returns all parts, laid end to end along the dimension named above; an argument that names none is the same for every part.
All inputs are finite; a program needn't handle non-finite values.
Results may differ from the reference program's by a relative error of at most 0.0083589.
Values are sent between devices in bfloat16 or wider.
A program may use at most 768 MiB of HBM per device.

```python
import jax
import jax.numpy as jnp
from jax import lax

B = 6
IMG = 448
PATCH = 14
D = 1152
HEADS = 16
HEAD = 72
FF = 4304

GRID = IMG // PATCH
TOKENS = GRID * GRID
PATCH_DIM = PATCH * PATCH * 3
LN_EPS = 1e-6


def draw_normal(rng_key, arr_shape, std_dev):
    return jax.random.normal(rng_key, arr_shape, jnp.float32) * std_dev


def smooth_images(base_key, num_images):
    key_freq, key_phase, key_amp, key_noise = jax.random.split(base_key, 4)
    wave_freq = jax.random.uniform(key_freq, (num_images, 8, 2), jnp.float32, -4.0, 4.0) * (2.0 * jnp.pi / IMG)
    wave_phase = jax.random.uniform(key_phase, (num_images, 8, 3), jnp.float32, 0.0, 2.0 * jnp.pi)
    wave_amp = draw_normal(key_amp, (num_images, 8, 3), 0.5)
    coords = jnp.arange(IMG, dtype=jnp.float32)
    row_angle = wave_freq[:, :, 0, None] * coords
    col_angle = wave_freq[:, :, 1, None, None] * coords[:, None] + wave_phase[:, :, None, :]
    waves = (jnp.einsum('nky,nkxc->nyxc', jnp.cos(row_angle), wave_amp[:, :, None, :] * jnp.cos(col_angle))
             - jnp.einsum('nky,nkxc->nyxc', jnp.sin(row_angle), wave_amp[:, :, None, :] * jnp.sin(col_angle)))
    return waves + draw_normal(key_noise, (num_images, IMG, IMG, 3), 0.2)


def setup_inputs(seed: int = 0, part: int = 0) -> dict:
    sub_keys = jax.random.split(jax.random.key(seed), 16)
    qk_gain = jnp.array([1.5, 1.5, 1.0], jnp.float32)[None, :, None, None]
    return {
        'images': smooth_images(jax.random.fold_in(sub_keys[0], part), B),
        'w_patch': draw_normal(sub_keys[1], (PATCH, PATCH, 3, D), PATCH_DIM ** -0.5).astype(jnp.bfloat16),
        'b_patch': draw_normal(sub_keys[2], (D,), 0.5),
        'pos_embed': draw_normal(sub_keys[3], (TOKENS, D), 1.0).astype(jnp.bfloat16),
        'ln1_gain': 1.0 + draw_normal(sub_keys[4], (D,), 0.2),
        'ln1_bias': draw_normal(sub_keys[5], (D,), 0.5),
        'w_qkv': (draw_normal(sub_keys[6], (D, 3, HEADS, HEAD), D ** -0.5) * qk_gain).astype(jnp.bfloat16),
        'b_qkv': draw_normal(sub_keys[7], (3, HEADS, HEAD), 0.5),
        'w_out': draw_normal(sub_keys[8], (HEADS, HEAD, D), 2.0 * D ** -0.5).astype(jnp.bfloat16),
        'b_out': draw_normal(sub_keys[9], (D,), 0.5),
        'ln2_gain': 1.0 + draw_normal(sub_keys[10], (D,), 0.2),
        'ln2_bias': draw_normal(sub_keys[11], (D,), 0.5),
        'w_fc1': draw_normal(sub_keys[12], (D, FF), D ** -0.5).astype(jnp.bfloat16),
        'b_fc1': draw_normal(sub_keys[13], (FF,), 0.5),
        'w_fc2': draw_normal(sub_keys[14], (FF, D), 1.5 * FF ** -0.5).astype(jnp.bfloat16),
        'b_fc2': draw_normal(sub_keys[15], (D,), 0.5),
    }


def layer_norm(x_in, ln_gain, ln_bias):
    row_mean = jnp.mean(x_in, axis=-1, keepdims=True)
    centered = x_in - row_mean
    variance = jnp.mean(centered * centered, axis=-1, keepdims=True)
    return centered * lax.rsqrt(variance + LN_EPS) * ln_gain + ln_bias


def reference(images, w_patch, b_patch, pos_embed, ln1_gain, ln1_bias, w_qkv, b_qkv, w_out, b_out, ln2_gain, ln2_bias, w_fc1, b_fc1, w_fc2, b_fc2):
    w_patch_flat = w_patch.reshape(PATCH_DIM, D)
    w_qkv_flat = w_qkv.reshape(D, 3 * D)
    b_qkv_flat = b_qkv.reshape(3 * D)
    w_out_flat = w_out.reshape(D, D)
    pos_f32 = pos_embed.astype(jnp.float32)

    def encode_image(single_image):
        pixels = single_image.astype(jnp.bfloat16).reshape(GRID, PATCH, GRID, PATCH, 3)
        patches = jnp.transpose(pixels, (0, 2, 1, 3, 4)).reshape(TOKENS, PATCH_DIM)
        patch_embed = jnp.dot(patches, w_patch_flat, preferred_element_type=jnp.float32)
        x_zero = (patch_embed + b_patch + pos_f32).astype(jnp.bfloat16)
        normed = layer_norm(x_zero.astype(jnp.float32), ln1_gain, ln1_bias).astype(jnp.bfloat16)
        qkv_proj = (jnp.dot(normed, w_qkv_flat, preferred_element_type=jnp.float32) + b_qkv_flat).astype(jnp.bfloat16)
        queries = qkv_proj[:, :D].reshape(GRID, GRID, HEADS, HEAD)
        keys_all = qkv_proj[:, D:2 * D].reshape(TOKENS, HEADS, HEAD).astype(jnp.float32)
        values_all = qkv_proj[:, 2 * D:].reshape(TOKENS, HEADS, HEAD).astype(jnp.float32)

        def attend_row(row_queries):
            scores = jnp.einsum('qhe,khe->hqk', row_queries.astype(jnp.float32), keys_all) * HEAD ** -0.5
            weights = jax.nn.softmax(scores, axis=-1).astype(jnp.bfloat16).astype(jnp.float32)
            return jnp.einsum('hqk,khe->qhe', weights, values_all).astype(jnp.bfloat16)

        attended = lax.map(attend_row, queries).reshape(TOKENS, D)
        residual = x_zero.astype(jnp.float32) + jnp.dot(attended, w_out_flat, preferred_element_type=jnp.float32) + b_out
        normed_two = layer_norm(residual, ln2_gain, ln2_bias).astype(jnp.bfloat16)
        hidden = jax.nn.gelu(jnp.dot(normed_two, w_fc1, preferred_element_type=jnp.float32) + b_fc1, approximate=True).astype(jnp.bfloat16)
        return (residual + jnp.dot(hidden, w_fc2, preferred_element_type=jnp.float32) + b_fc2).astype(jnp.bfloat16)

    return lax.map(encode_image, images)
```

```python
import functools
import math
import jax
import jax.numpy as jnp
from jax import lax
from jax.experimental import pallas as pl
from jax.experimental.pallas import tpu as pltpu
from jax.sharding import PartitionSpec as P

LN_EPS = 1e-6
MESH = pl.DeviceIdType.MESH
F32 = jnp.float32
BF16 = jnp.bfloat16


def layer_norm(x_in, ln_gain, ln_bias):
    row_mean = jnp.mean(x_in, axis=-1, keepdims=True)
    centered = x_in - row_mean
    variance = jnp.mean(centered * centered, axis=-1, keepdims=True)
    return centered * lax.rsqrt(variance + LN_EPS) * ln_gain + ln_bias


def embed_tokens(images, w_patch, b_patch, pos_embed):
    num_images, num_rows, num_cols, channels = images.shape
    patch_len = w_patch.shape[0]
    patch_embed = lax.conv_general_dilated(
        images.astype(BF16), w_patch, (patch_len, patch_len), 'VALID',
        dimension_numbers=('NHWC', 'HWIO', 'NHWC'), preferred_element_type=F32)
    patch_embed = patch_embed.reshape(num_images, -1, w_patch.shape[3])
    return (patch_embed + b_patch + pos_embed.astype(F32)).astype(BF16)


def attend_kernel(n_chip, scale, y_ref, bias_ref, w_hbm, o_out,
                  y_b, y_a, w_b, w_a, q_b, k_b, v_b, q_a, k_a, v_a, s_buf, m_buf, o_b, o_a,
                  w_sem, y_send, y_recv, f_send, f_recv, o_send, o_recv):
    me = lax.axis_index('sp')
    chip = me // 2
    core = lax.rem(me, 2)
    sib = chip * 2 + (1 - core)
    heads_b, heads_a = w_b.shape[1] // 72, w_a.shape[1] // 72
    dim = y_ref.shape[2]
    n_dev = 2 * n_chip
    odd = lax.rem(chip, 2)
    half = chip // 2

    def image_of(owner, unit):
        first = (owner // 2) * 3
        return first + 1 if unit == 0 else first + 2 * lax.rem(owner, 2)

    head_b = (odd * 2 + core) * heads_b
    head_a = core * heads_a

    w_copies = []
    for t in range(3):
        for u, (w_s, h0) in enumerate(((w_b, head_b), (w_a, head_a))):
            rows = w_s.shape[1]
            c = pltpu.make_async_copy(
                w_hbm.at[pl.ds(pl.multiple_of(t * dim + h0 * 72, 8), rows)], w_s.at[t], w_sem.at[u, t])
            c.start()
            w_copies.append((u, c))

    barrier = pltpu.get_barrier_semaphore()
    for j in range(1, n_dev):
        pl.semaphore_signal(barrier, inc=1, device_id={'sp': lax.rem(me + j, n_dev)}, device_id_type=MESH)
    pl.semaphore_wait(barrier, n_dev - 1)

    offs = (0, 1, 3, 2)
    back = {0: 0, 1: 2, 2: 1, 3: 3}
    y_units = (y_b, y_a)
    sends = []
    for u in range(2):
        for j in range(1, n_chip):
            owner = lax.rem(chip + offs[j], n_chip)
            dst = y_units[u].at[back[j], core]
            c = pltpu.make_async_remote_copy(
                y_ref.at[image_of(owner, u)], dst, y_send.at[u, j], y_recv.at[u, back[j]],
                device_id={'sp': owner * 2 + core}, device_id_type=MESH)
            c.start()
            sends.append(c)
    forwards = {}
    for u in range(2):
        c = pltpu.make_async_remote_copy(
            y_ref.at[image_of(chip, u)], y_units[u].at[0, core], f_send.at[u, 0], f_recv.at[u, 0],
            device_id={'sp': sib}, device_id_type=MESH)
        c.start()
        forwards[u, 0] = c
    for u in range(2):
        y_units[u][0, core] = y_ref[image_of(chip, u)]

    def recv_copy(u, j):
        return pltpu.make_async_remote_copy(
            y_ref.at[0], y_units[u].at[j, core], y_send.at[u, 1], y_recv.at[u, j],
            device_id={'sp': sib}, device_id_type=MESH)

    def project(u, j):
        y_u = y_units[u]
        w_u = (w_b, w_a)[u]
        qkv = ((q_b, k_b, v_b), (q_a, k_a, v_a))[u]
        heads = (heads_b, heads_a)[u]
        h0 = (head_b, head_a)[u]
        y_chunk = y_u[j].reshape(256, dim)
        step = 4
        for t in range(3):
            for g in range(0, heads, step):
                prod = lax.dot_general(w_u[t, g * 72:(g + step) * 72], y_chunk, (((1,), (1,)), ((), ())),
                                       preferred_element_type=F32)
                for h in range(step):
                    row0 = pl.multiple_of(t * dim + (h0 + g + h) * 72, 8)
                    val = prod[h * 72:(h + 1) * 72] + bias_ref[pl.ds(row0, 72)]
                    if t == 1:
                        qkv[t][g + h, 256 * j:256 * (j + 1), :] = val.T.astype(BF16)
                    else:
                        qkv[t][g + h, :, 256 * j:256 * (j + 1)] = val.astype(BF16)

    def scores(u, item, slot):
        q_u, k_u = ((q_b, k_b), (q_a, k_a))[u]
        h = item // n_chip
        blk = pl.ds(pl.multiple_of(lax.rem(item, n_chip) * 256, 256), 256)
        s = jnp.dot(k_u[h], q_u[h, :, blk], preferred_element_type=F32)
        s_buf[slot] = s
        m_buf[slot] = jnp.broadcast_to(jnp.max(s, axis=0, keepdims=True), (8, 256))

    def weigh(u, item, slot):
        v_u = (v_b, v_a)[u]
        o_u = (o_b, o_a)[u]
        h = item // n_chip
        j = lax.rem(item, n_chip)
        e = jnp.exp2((s_buf[slot] - m_buf[slot][:1]) * scale)
        total = jnp.sum(e, axis=0, keepdims=True)
        o = jnp.dot(v_u[h], e.astype(BF16), preferred_element_type=F32) * (1.0 / total)
        o = o.astype(BF16)
        o_u[j, 0, h] = o[:, :128]
        o_u[j, 1, h] = o[:, 128:]

    def attend(u, first, last):
        scores(u, first, 0)

        def body(i, carry):
            item = first + 2 * i
            scores(u, item + 1, 1)
            weigh(u, item, 0)
            scores(u, lax.min(item + 2, last - 1), 0)
            weigh(u, item + 1, 1)
            return carry

        lax.fori_loop(0, (last - first) // 2, body, 0)

    out_sends = []

    def send_out(u, g, g0, heads_out):
        o_u = (o_b, o_a)[u]
        h0 = (head_b, head_a)[u]
        for j in range(n_chip):
            owner = lax.rem(chip + offs[j], n_chip)
            for c2 in range(2):
                dst_core = core if c2 == 0 else 1 - core
                src = o_u.at[j, dst_core, pl.ds(g0, heads_out)]
                dst = o_out.at[image_of(chip, u), pl.ds(h0 + g0, heads_out)]
                if j == 0 and c2 == 0:
                    c = pltpu.make_async_copy(src, dst, o_recv.at[g, 0, 0])
                else:
                    c = pltpu.make_async_remote_copy(
                        src, dst, o_send.at[g, j, c2], o_recv.at[g, back[j], c2],
                        device_id={'sp': owner * 2 + dst_core}, device_id_type=MESH)
                c.start()
                out_sends.append((c, j == 0 and c2 == 0))

    for u in range(2):
        for uu, c in w_copies:
            if uu == u:
                c.wait()
        for j in range(n_chip):
            if j > 0:
                recv_copy(u, j).wait_recv()
                f = pltpu.make_async_remote_copy(
                    y_units[u].at[j, core], y_units[u].at[j, core], f_send.at[u, j], f_recv.at[u, j],
                    device_id={'sp': sib}, device_id_type=MESH)
                f.start()
                forwards[u, j] = f
            pltpu.make_async_remote_copy(
                y_units[u].at[j, core], y_units[u].at[j, 1 - core], f_send.at[u, j], f_recv.at[u, j],
                device_id={'sp': sib}, device_id_type=MESH).wait_recv()
            project(u, j)
        if u == 0:
            attend(u, 0, heads_b * n_chip)
            send_out(u, 0, 0, heads_b)
        else:
            attend(u, 0, heads_b * n_chip)
            send_out(u, 1, 0, heads_b)
            attend(u, heads_b * n_chip, heads_a * n_chip)
            send_out(u, 2, heads_b, heads_a - heads_b)

    for c in sends:
        c.wait_send()
    for c in forwards.values():
        c.wait_send()
    for c, local in out_sends:
        if local:
            c.wait()
        else:
            c.wait_send()
    for g in range(3):
        u = 0 if g == 0 else 1
        nh = heads_b if g < 2 else heads_a - heads_b
        for j in range(n_chip):
            for c2 in range(2):
                if j == 0 and c2 == 0:
                    continue
                src_chip = lax.rem(chip + offs[j], n_chip)
                src_core = core if c2 == 0 else 1 - core
                if u == 0:
                    h_src = (lax.rem(src_chip, 2) * 2 + src_core) * heads_b
                else:
                    h_src = src_core * heads_a + (0 if g == 1 else heads_b)
                pltpu.make_async_remote_copy(
                    (o_b, o_a)[u].at[0, 0, pl.ds(0, nh)], o_out.at[image_of(src_chip, u), pl.ds(h_src, nh)],
                    o_send.at[g, j, c2], o_recv.at[g, j, c2],
                    device_id={'sp': sib}, device_id_type=MESH).wait_recv()


def attend_layer(normed, w_qkv_t, bias_col, n_dev, num_heads, head_dim):
    images, band, dim = normed.shape
    n_chip = n_dev // 2
    heads_b, heads_a = num_heads // 4, num_heads // 2
    keys = band * n_dev
    scale = head_dim ** -0.5 * math.log2(math.e)

    def unit(heads):
        return [pltpu.VMEM((heads, head_dim, keys), BF16), pltpu.VMEM((heads, keys, head_dim), BF16),
                pltpu.VMEM((heads, head_dim, keys), BF16)]

    vmem = pl.BlockSpec(memory_space=pltpu.VMEM)
    hbm = pl.BlockSpec(memory_space=pl.ANY)
    dma = pltpu.SemaphoreType.DMA
    return pl.pallas_call(
        functools.partial(attend_kernel, n_chip, scale),
        out_shape=jax.ShapeDtypeStruct((images, num_heads, head_dim, band), BF16),
        in_specs=[vmem, vmem, hbm],
        out_specs=hbm,
        scratch_shapes=[
            pltpu.VMEM((n_chip, 2, band, dim), BF16), pltpu.VMEM((n_chip, 2, band, dim), BF16),
            pltpu.VMEM((3, heads_b * head_dim, dim), BF16), pltpu.VMEM((3, heads_a * head_dim, dim), BF16),
            *unit(heads_b), *unit(heads_a),
            pltpu.VMEM((2, keys, 256), F32), pltpu.VMEM((2, 8, 256), F32),
            pltpu.VMEM((n_chip, 2, heads_b, head_dim, band), BF16),
            pltpu.VMEM((n_chip, 2, heads_a, head_dim, band), BF16),
            dma((2, 3)), dma((2, n_chip)), dma((2, n_chip)), dma((2, n_chip)), dma((2, n_chip)),
            dma((3, n_chip, 2)), dma((3, n_chip, 2)),
        ],
        compiler_params=pltpu.CompilerParams(collective_id=0, has_side_effects=True, vmem_limit_bytes=50 * 2**20),
        name='attend',
    )(normed, bias_col, w_qkv_t)


def mlp_kernel(chunk, tail, o_ref, x_ref, wo_ref, bo_ref, g2_ref, c2_ref, b1_ref, b2_ref, w1_hbm, w2_hbm, out_ref,
               w1, w2, acc, y2, hid, sem1, sem2):
    n_full = (w1.shape[0] - tail) // chunk

    def w_copy(i, size):
        rows = pl.ds(i * chunk, size) if isinstance(i, int) else pl.ds(pl.multiple_of(i * chunk, chunk), size)
        return (pltpu.make_async_copy(w1_hbm.at[rows], w1.at[rows], sem1.at[i]),
                pltpu.make_async_copy(w2_hbm.at[rows], w2.at[rows], sem2.at[i]))

    for i in range(n_full + 1):
        for c in w_copy(i, chunk if i < n_full else tail):
            c.start()
    n_img, band = o_ref.shape[0], o_ref.shape[2]

    def proj(i, carry):
        rows = pl.ds(pl.multiple_of(i * band, band), band)
        r = lax.dot_general(o_ref[i], wo_ref[...], (((0,), (0,)), ((), ())), preferred_element_type=F32)
        r = x_ref[rows].astype(F32) + r + bo_ref[...]
        acc[rows] = r + b2_ref[...]
        y2[rows] = layer_norm(r, g2_ref[...], c2_ref[...]).astype(BF16)
        return carry

    lax.fori_loop(0, n_img, proj, 0)

    def first(i, size, slot):
        rows = pl.ds(i * chunk, size) if isinstance(i, int) else pl.ds(pl.multiple_of(i * chunk, chunk), size)
        pre = lax.dot_general(y2[...], w1[rows], (((1,), (1,)), ((), ())), preferred_element_type=F32)
        pre = pre + b1_ref[:, rows]
        hid[slot, :, :size] = jax.nn.gelu(pre, approximate=True).astype(BF16)

    def second(i, size, slot):
        rows = pl.ds(i * chunk, size) if isinstance(i, int) else pl.ds(pl.multiple_of(i * chunk, chunk), size)
        acc[...] += jnp.dot(hid[slot, :, :size], w2[rows], preferred_element_type=F32)

    w_copy(0, chunk)[0].wait()
    first(0, chunk, 0)

    def body(i, carry):
        w_copy(i + 1, chunk)[0].wait()
        w_copy(i, chunk)[1].wait()
        first(i + 1, chunk, lax.rem(i + 1, 2))
        second(i, chunk, lax.rem(i, 2))
        return carry

    lax.fori_loop(0, n_full - 1, body, 0)
    w_copy(n_full, tail)[0].wait()
    w_copy(n_full - 1, chunk)[1].wait()
    first(n_full, tail, n_full % 2)
    second(n_full - 1, chunk, (n_full - 1) % 2)
    w_copy(n_full, tail)[1].wait()
    second(n_full, tail, n_full % 2)
    out_ref[...] = acc[...].astype(BF16)


def mlp_layer(o_t, x_zero, w_out, b_out, ln2_gain, ln2_bias, w_fc1_t, b_fc1, w_fc2, b_fc2):
    images, dim, band = o_t.shape
    ff = w_fc2.shape[0]
    rows = images * band
    chunk = 512
    tail = ff - (ff - 1) // chunk * chunk
    n_chunks = (ff - tail) // chunk + 1
    vmem = pl.BlockSpec(memory_space=pltpu.VMEM)
    hbm = pl.BlockSpec(memory_space=pl.ANY)
    flops = 2 * rows * dim * (dim + 2 * ff)
    return pl.pallas_call(
        functools.partial(mlp_kernel, chunk, tail),
        out_shape=jax.ShapeDtypeStruct((rows, dim), BF16),
        in_specs=[vmem] * 8 + [hbm, hbm],
        out_specs=vmem,
        scratch_shapes=[
            pltpu.VMEM((ff, dim), BF16), pltpu.VMEM((ff, dim), BF16), pltpu.VMEM((rows, dim), F32),
            pltpu.VMEM((rows, dim), BF16), pltpu.VMEM((2, rows, chunk), BF16),
            pltpu.SemaphoreType.DMA((n_chunks,)), pltpu.SemaphoreType.DMA((n_chunks,)),
        ],
        compiler_params=pltpu.CompilerParams(vmem_limit_bytes=56 * 2**20),
        cost_estimate=pl.CostEstimate(flops=flops, bytes_accessed=32 * 2**20, transcendentals=0),
        name='mlp',
    )(o_t, x_zero, w_out, b_out[None], ln2_gain[None], ln2_bias[None], b_fc1[None], b_fc2[None], w_fc1_t, w_fc2)


def solution(mesh):
    n_dev = mesh.shape['sp']

    def device_step(images, w_patch, b_patch, pos_embed, ln1_gain, ln1_bias, w_qkv, b_qkv, w_out, b_out, ln2_gain, ln2_bias, w_fc1, b_fc1, w_fc2, b_fc2):
        dim, _, num_heads, head_dim = w_qkv.shape
        x_zero = embed_tokens(images, w_patch, b_patch, pos_embed)
        normed = layer_norm(x_zero.astype(F32), ln1_gain, ln1_bias).astype(BF16)
        w_qkv_t = jnp.transpose(w_qkv, (1, 2, 3, 0)).reshape(3 * dim, dim)
        o_t = attend_layer(normed, w_qkv_t, b_qkv.reshape(3 * dim, 1), n_dev, num_heads, head_dim)
        num_images, band = normed.shape[:2]
        out = mlp_layer(o_t.reshape(num_images, dim, band), x_zero.reshape(num_images * band, dim), w_out.reshape(dim, dim),
                        b_out, ln2_gain, ln2_bias, w_fc1.T, b_fc1, w_fc2, b_fc2)
        return out.reshape(num_images, band, dim)

    in_specs = (P('dp', 'sp', None, None), P(), P(), P('sp', None), P(), P(), P(), P(), P(), P(), P(), P(), P(), P(), P(), P())
    return jax.shard_map(device_step, mesh=mesh, in_specs=in_specs, out_specs=P('dp', 'sp', None), check_vma=False)
```

```python
import functools
import math
import jax
import jax.numpy as jnp
import numpy as np
from jax import lax
from jax.experimental import pallas as pl
from jax.experimental.pallas import tpu as pltpu
from jax.sharding import PartitionSpec as P

LN_EPS = 1e-6
MESH = pl.DeviceIdType.MESH
F32 = jnp.float32
BF16 = jnp.bfloat16


def layer_norm(x_in, ln_gain, ln_bias):
    row_mean = jnp.mean(x_in, axis=-1, keepdims=True)
    centered = x_in - row_mean
    variance = jnp.mean(centered * centered, axis=-1, keepdims=True)
    return centered * lax.rsqrt(variance + LN_EPS) * ln_gain + ln_bias


def embed_kernel(patch, img_ref, w_ref, sel_ref, pos_ref, bp_ref, g1_ref, c1_ref, x_out, y_out,
                 w_f, w_s, rows_s, perm_s, x_t):
    n_img, chan, height, width = img_ref.shape
    cols = width // patch
    grid_rows = height // patch
    slab = sel_ref.shape[0] // grid_rows
    band = grid_rows * cols
    lanes = 128
    per_tile = lanes // cols

    def weights(n, carry):
        tile = pl.ds(pl.multiple_of(n * lanes, lanes), lanes)
        for q in range(patch):
            w_f[n, q * slab + slab - 8:(q + 1) * slab] = jnp.zeros((8, lanes), F32)
        for p in range(patch):
            for c in range(chan):
                w_f[n, pl.ds(c * patch + p, patch, stride=slab), :] = w_ref[p, c, :, tile].astype(F32)
        w_s[:, tile] = w_f[n].astype(BF16)
        return carry

    lax.fori_loop(0, w_f.shape[0], weights, 0)

    out_col = lax.broadcasted_iota(jnp.int32, (1, width), 1)
    source = lax.rem(out_col, cols) * patch + out_col // cols
    perm_s[...] = jnp.where(lax.broadcasted_iota(jnp.int32, (width, width), 0) == source, 1.0, 0.0).astype(BF16)
    for i in range(n_img):
        pixels = img_ref[i].reshape(chan * height, width).astype(BF16)
        rows_s[i] = jnp.dot(sel_ref[...], pixels, preferred_element_type=F32).astype(BF16)

    lane_group = lax.broadcasted_iota(jnp.int32, (slab, lanes), 1) // cols

    def patches(i, carry):
        z = jnp.dot(rows_s[i], perm_s[...], preferred_element_type=F32)
        z = jnp.concatenate([z, jnp.zeros((z.shape[0], -width % lanes), F32)], axis=1)
        for q in range(patch):
            tile, off = q // per_tile, q % per_tile
            block = jnp.zeros((slab, lanes), F32)
            for y in range(grid_rows):
                part = z[y * slab:(y + 1) * slab, tile * lanes:(tile + 1) * lanes]
                shift = (y - off) % per_tile * cols
                if shift:
                    part = pltpu.roll(part, shift, 1)
                block = jnp.where(lane_group == y, part, block)
            x_t[i, q * slab:(q + 1) * slab] = block.astype(BF16)
        return carry

    lax.fori_loop(0, n_img, patches, 0)

    def embed(i, carry):
        x0 = lax.dot_general(x_t[i], w_s[...], (((0,), (0,)), ((), ())), preferred_element_type=F32)
        x0 = (x0 + bp_ref[...] + pos_ref[...].astype(F32)).astype(BF16)
        x_out[i] = x0
        y_out[i] = layer_norm(x0.astype(F32), g1_ref[...], c1_ref[...]).astype(BF16)
        return carry

    lax.fori_loop(0, n_img, embed, 0)


def embed_tokens(images, w_patch, b_patch, pos_embed, ln1_gain, ln1_bias):
    n_img, height, width, chan = images.shape
    patch, dim = w_patch.shape[0], w_patch.shape[3]
    grid_rows = height // patch
    band = pos_embed.shape[0]
    slab = -(-chan * patch // 16) * 16
    select = np.zeros((grid_rows * slab, chan * height), np.float32)
    for y in range(grid_rows):
        for c in range(chan):
            for p in range(patch):
                select[y * slab + c * patch + p, c * height + y * patch + p] = 1.0
    vmem = pl.BlockSpec(memory_space=pltpu.VMEM)
    depth = patch * slab
    return pl.pallas_call(
        functools.partial(embed_kernel, patch),
        out_shape=[jax.ShapeDtypeStruct((n_img, band, dim), BF16)] * 2,
        in_specs=[vmem] * 7,
        out_specs=[vmem] * 2,
        scratch_shapes=[
            pltpu.VMEM((dim // 128, depth, 128), F32), pltpu.VMEM((depth, dim), BF16),
            pltpu.VMEM((n_img, grid_rows * slab, width), BF16), pltpu.VMEM((width, width), BF16),
            pltpu.VMEM((n_img, depth, band), BF16),
        ],
        compiler_params=pltpu.CompilerParams(vmem_limit_bytes=32 * 2**20),
        name='embed',
    )(jnp.transpose(images, (0, 3, 1, 2)), jnp.transpose(w_patch, (0, 2, 1, 3)), jnp.asarray(select, BF16), pos_embed,
      b_patch[None], ln1_gain[None], ln1_bias[None])


def attend_kernel(n_chip, scale, y_ref, bias_ref, w_hbm, o_out,
                  y_b, y_a, w_b, w_a, q_b, k_b, v_b, q_a, k_a, v_a, s_buf, m_buf, o_b, o_a,
                  w_sem, y_send, y_recv, f_send, f_recv, o_send, o_recv):
    me = lax.axis_index('sp')
    chip = me // 2
    core = lax.rem(me, 2)
    sib = chip * 2 + (1 - core)
    heads_b, heads_a = w_b.shape[1] // 72, w_a.shape[1] // 72
    dim = y_ref.shape[2]
    n_dev = 2 * n_chip
    odd = lax.rem(chip, 2)
    half = chip // 2

    def image_of(owner, unit):
        first = (owner // 2) * 3
        return first + 1 if unit == 0 else first + 2 * lax.rem(owner, 2)

    head_b = (odd * 2 + core) * heads_b
    head_a = core * heads_a

    w_copies = []
    for t in range(3):
        for u, (w_s, h0) in enumerate(((w_b, head_b), (w_a, head_a))):
            rows = w_s.shape[1]
            c = pltpu.make_async_copy(
                w_hbm.at[pl.ds(pl.multiple_of(t * dim + h0 * 72, 8), rows)], w_s.at[t], w_sem.at[u, t])
            c.start()
            w_copies.append((u, c))

    barrier = pltpu.get_barrier_semaphore()
    for j in range(1, n_dev):
        pl.semaphore_signal(barrier, inc=1, device_id={'sp': lax.rem(me + j, n_dev)}, device_id_type=MESH)
    pl.semaphore_wait(barrier, n_dev - 1)

    offs = (0, 1, 3, 2)
    back = {0: 0, 1: 2, 2: 1, 3: 3}
    y_units = (y_b, y_a)
    sends = []
    for u in range(2):
        for j in range(1, n_chip):
            owner = lax.rem(chip + offs[j], n_chip)
            dst = y_units[u].at[back[j], core]
            c = pltpu.make_async_remote_copy(
                y_ref.at[image_of(owner, u)], dst, y_send.at[u, j], y_recv.at[u, back[j]],
                device_id={'sp': owner * 2 + core}, device_id_type=MESH)
            c.start()
            sends.append(c)
    forwards = {}
    for u in range(2):
        c = pltpu.make_async_remote_copy(
            y_ref.at[image_of(chip, u)], y_units[u].at[0, core], f_send.at[u, 0], f_recv.at[u, 0],
            device_id={'sp': sib}, device_id_type=MESH)
        c.start()
        forwards[u, 0] = c
    for u in range(2):
        y_units[u][0, core] = y_ref[image_of(chip, u)]

    def recv_copy(u, j):
        return pltpu.make_async_remote_copy(
            y_ref.at[0], y_units[u].at[j, core], y_send.at[u, 1], y_recv.at[u, j],
            device_id={'sp': sib}, device_id_type=MESH)

    def project(u, j):
        y_u = y_units[u]
        w_u = (w_b, w_a)[u]
        qkv = ((q_b, k_b, v_b), (q_a, k_a, v_a))[u]
        heads = (heads_b, heads_a)[u]
        h0 = (head_b, head_a)[u]
        y_chunk = y_u[j].reshape(256, dim)
        step = 4
        for t in range(3):
            for g in range(0, heads, step):
                prod = lax.dot_general(w_u[t, g * 72:(g + step) * 72], y_chunk, (((1,), (1,)), ((), ())),
                                       preferred_element_type=F32)
                bias = bias_ref[t, pl.ds(h0 + g, step)].T
                for h in range(step):
                    val = prod[h * 72:(h + 1) * 72] + bias[:, h:h + 1]
                    if t == 1:
                        qkv[t][g + h, 256 * j:256 * (j + 1), :] = val.T.astype(BF16)
                    else:
                        qkv[t][g + h, :, 256 * j:256 * (j + 1)] = val.astype(BF16)

    def scores(u, item, slot):
        q_u, k_u = ((q_b, k_b), (q_a, k_a))[u]
        h = item // n_chip
        blk = pl.ds(pl.multiple_of(lax.rem(item, n_chip) * 256, 256), 256)
        s = jnp.dot(k_u[h], q_u[h, :, blk], preferred_element_type=F32)
        s_buf[slot] = s
        m_buf[slot] = jnp.broadcast_to(jnp.max(s, axis=0, keepdims=True), (8, 256))

    def weigh(u, item, slot):
        v_u = (v_b, v_a)[u]
        o_u = (o_b, o_a)[u]
        h = item // n_chip
        j = lax.rem(item, n_chip)
        e = jnp.exp2((s_buf[slot] - m_buf[slot][:1]) * scale)
        total = jnp.sum(e, axis=0, keepdims=True)
        o = jnp.dot(v_u[h], e.astype(BF16), preferred_element_type=F32) * (1.0 / total)
        o = o.astype(BF16)
        o_u[j, 0, h] = o[:, :128]
        o_u[j, 1, h] = o[:, 128:]

    def attend(u, first, last):
        scores(u, first, 0)

        def body(i, carry):
            item = first + 2 * i
            scores(u, item + 1, 1)
            weigh(u, item, 0)
            scores(u, lax.min(item + 2, last - 1), 0)
            weigh(u, item + 1, 1)
            return carry

        lax.fori_loop(0, (last - first) // 2, body, 0)

    out_sends = []

    def send_out(u, g, g0, heads_out):
        o_u = (o_b, o_a)[u]
        h0 = (head_b, head_a)[u]
        for j in range(n_chip):
            owner = lax.rem(chip + offs[j], n_chip)
            for c2 in range(2):
                dst_core = core if c2 == 0 else 1 - core
                src = o_u.at[j, dst_core, pl.ds(g0, heads_out)]
                dst = o_out.at[image_of(chip, u), pl.ds(h0 + g0, heads_out)]
                if j == 0 and c2 == 0:
                    c = pltpu.make_async_copy(src, dst, o_recv.at[g, 0, 0])
                else:
                    c = pltpu.make_async_remote_copy(
                        src, dst, o_send.at[g, j, c2], o_recv.at[g, back[j], c2],
                        device_id={'sp': owner * 2 + dst_core}, device_id_type=MESH)
                c.start()
                out_sends.append((c, j == 0 and c2 == 0))

    for u in range(2):
        for uu, c in w_copies:
            if uu == u:
                c.wait()
        for j in range(n_chip):
            if j > 0:
                recv_copy(u, j).wait_recv()
                f = pltpu.make_async_remote_copy(
                    y_units[u].at[j, core], y_units[u].at[j, core], f_send.at[u, j], f_recv.at[u, j],
                    device_id={'sp': sib}, device_id_type=MESH)
                f.start()
                forwards[u, j] = f
            pltpu.make_async_remote_copy(
                y_units[u].at[j, core], y_units[u].at[j, 1 - core], f_send.at[u, j], f_recv.at[u, j],
                device_id={'sp': sib}, device_id_type=MESH).wait_recv()
            project(u, j)
        if u == 0:
            attend(u, 0, heads_b * n_chip)
            send_out(u, 0, 0, heads_b)
        else:
            attend(u, 0, heads_b * n_chip)
            send_out(u, 1, 0, heads_b)
            attend(u, heads_b * n_chip, heads_a * n_chip)
            send_out(u, 2, heads_b, heads_a - heads_b)

    for c in sends:
        c.wait_send()
    for c in forwards.values():
        c.wait_send()
    for c, local in out_sends:
        if local:
            c.wait()
        else:
            c.wait_send()
    for g in range(3):
        u = 0 if g == 0 else 1
        nh = heads_b if g < 2 else heads_a - heads_b
        for j in range(n_chip):
            for c2 in range(2):
                if j == 0 and c2 == 0:
                    continue
                src_chip = lax.rem(chip + offs[j], n_chip)
                src_core = core if c2 == 0 else 1 - core
                if u == 0:
                    h_src = (lax.rem(src_chip, 2) * 2 + src_core) * heads_b
                else:
                    h_src = src_core * heads_a + (0 if g == 1 else heads_b)
                pltpu.make_async_remote_copy(
                    (o_b, o_a)[u].at[0, 0, pl.ds(0, nh)], o_out.at[image_of(src_chip, u), pl.ds(h_src, nh)],
                    o_send.at[g, j, c2], o_recv.at[g, j, c2],
                    device_id={'sp': sib}, device_id_type=MESH).wait_recv()


def attend_layer(normed, w_qkv_t, b_qkv, n_dev, num_heads, head_dim):
    images, band, dim = normed.shape
    n_chip = n_dev // 2
    heads_b, heads_a = num_heads // 4, num_heads // 2
    keys = band * n_dev
    scale = head_dim ** -0.5 * math.log2(math.e)

    def unit(heads):
        return [pltpu.VMEM((heads, head_dim, keys), BF16), pltpu.VMEM((heads, keys, head_dim), BF16),
                pltpu.VMEM((heads, head_dim, keys), BF16)]

    vmem = pl.BlockSpec(memory_space=pltpu.VMEM)
    hbm = pl.BlockSpec(memory_space=pl.ANY)
    dma = pltpu.SemaphoreType.DMA
    return pl.pallas_call(
        functools.partial(attend_kernel, n_chip, scale),
        out_shape=jax.ShapeDtypeStruct((images, num_heads, head_dim, band), BF16),
        in_specs=[vmem, vmem, hbm],
        out_specs=hbm,
        scratch_shapes=[
            pltpu.VMEM((n_chip, 2, band, dim), BF16), pltpu.VMEM((n_chip, 2, band, dim), BF16),
            pltpu.VMEM((3, heads_b * head_dim, dim), BF16), pltpu.VMEM((3, heads_a * head_dim, dim), BF16),
            *unit(heads_b), *unit(heads_a),
            pltpu.VMEM((2, keys, 256), F32), pltpu.VMEM((2, 8, 256), F32),
            pltpu.VMEM((n_chip, 2, heads_b, head_dim, band), BF16),
            pltpu.VMEM((n_chip, 2, heads_a, head_dim, band), BF16),
            dma((2, 3)), dma((2, n_chip)), dma((2, n_chip)), dma((2, n_chip)), dma((2, n_chip)),
            dma((3, n_chip, 2)), dma((3, n_chip, 2)),
        ],
        compiler_params=pltpu.CompilerParams(collective_id=0, has_side_effects=True, vmem_limit_bytes=50 * 2**20),
        name='attend',
    )(normed, b_qkv, w_qkv_t)


def mlp_kernel(chunk, tail, o_ref, x_ref, wo_ref, bo_ref, g2_ref, c2_ref, b1_ref, b2_ref, w1_hbm, w2_hbm, out_ref,
               w1, w2, acc, y2, hid, sem1, sem2):
    n_full = (w1.shape[0] - tail) // chunk

    def w_copy(i, size):
        rows = pl.ds(i * chunk, size) if isinstance(i, int) else pl.ds(pl.multiple_of(i * chunk, chunk), size)
        return (pltpu.make_async_copy(w1_hbm.at[rows], w1.at[rows], sem1.at[i]),
                pltpu.make_async_copy(w2_hbm.at[rows], w2.at[rows], sem2.at[i]))

    for i in range(n_full + 1):
        for c in w_copy(i, chunk if i < n_full else tail):
            c.start()
    n_img, band = o_ref.shape[0], o_ref.shape[2]

    def proj(i, carry):
        rows = pl.ds(pl.multiple_of(i * band, band), band)
        r = lax.dot_general(o_ref[i], wo_ref[...], (((0,), (0,)), ((), ())), preferred_element_type=F32)
        r = x_ref[rows].astype(F32) + r + bo_ref[...]
        acc[rows] = r + b2_ref[...]
        y2[rows] = layer_norm(r, g2_ref[...], c2_ref[...]).astype(BF16)
        return carry

    lax.fori_loop(0, n_img, proj, 0)

    def first(i, size, slot):
        rows = pl.ds(i * chunk, size) if isinstance(i, int) else pl.ds(pl.multiple_of(i * chunk, chunk), size)
        pre = lax.dot_general(y2[...], w1[rows], (((1,), (1,)), ((), ())), preferred_element_type=F32)
        pre = pre + b1_ref[:, rows]
        hid[slot, :, :size] = jax.nn.gelu(pre, approximate=True).astype(BF16)

    def second(i, size, slot):
        rows = pl.ds(i * chunk, size) if isinstance(i, int) else pl.ds(pl.multiple_of(i * chunk, chunk), size)
        acc[...] += jnp.dot(hid[slot, :, :size], w2[rows], preferred_element_type=F32)

    w_copy(0, chunk)[0].wait()
    first(0, chunk, 0)

    def body(i, carry):
        w_copy(i + 1, chunk)[0].wait()
        w_copy(i, chunk)[1].wait()
        first(i + 1, chunk, lax.rem(i + 1, 2))
        second(i, chunk, lax.rem(i, 2))
        return carry

    lax.fori_loop(0, n_full - 1, body, 0)
    w_copy(n_full, tail)[0].wait()
    w_copy(n_full - 1, chunk)[1].wait()
    first(n_full, tail, n_full % 2)
    second(n_full - 1, chunk, (n_full - 1) % 2)
    w_copy(n_full, tail)[1].wait()
    second(n_full, tail, n_full % 2)
    out_ref[...] = acc[...].astype(BF16)


def mlp_layer(o_t, x_zero, w_out, b_out, ln2_gain, ln2_bias, w_fc1_t, b_fc1, w_fc2, b_fc2):
    images, dim, band = o_t.shape
    ff = w_fc2.shape[0]
    rows = images * band
    chunk = 512
    tail = ff - (ff - 1) // chunk * chunk
    n_chunks = (ff - tail) // chunk + 1
    vmem = pl.BlockSpec(memory_space=pltpu.VMEM)
    hbm = pl.BlockSpec(memory_space=pl.ANY)
    flops = 2 * rows * dim * (dim + 2 * ff)
    return pl.pallas_call(
        functools.partial(mlp_kernel, chunk, tail),
        out_shape=jax.ShapeDtypeStruct((rows, dim), BF16),
        in_specs=[vmem] * 8 + [hbm, hbm],
        out_specs=vmem,
        scratch_shapes=[
            pltpu.VMEM((ff, dim), BF16), pltpu.VMEM((ff, dim), BF16), pltpu.VMEM((rows, dim), F32),
            pltpu.VMEM((rows, dim), BF16), pltpu.VMEM((2, rows, chunk), BF16),
            pltpu.SemaphoreType.DMA((n_chunks,)), pltpu.SemaphoreType.DMA((n_chunks,)),
        ],
        compiler_params=pltpu.CompilerParams(vmem_limit_bytes=56 * 2**20),
        cost_estimate=pl.CostEstimate(flops=flops, bytes_accessed=32 * 2**20, transcendentals=0),
        name='mlp',
    )(o_t, x_zero, w_out, b_out[None], ln2_gain[None], ln2_bias[None], b_fc1[None], b_fc2[None], w_fc1_t, w_fc2)


def solution(mesh):
    n_dev = mesh.shape['sp']

    def device_step(images, w_patch, b_patch, pos_embed, ln1_gain, ln1_bias, w_qkv, b_qkv, w_out, b_out, ln2_gain, ln2_bias, w_fc1, b_fc1, w_fc2, b_fc2):
        dim, _, num_heads, head_dim = w_qkv.shape
        x_zero, normed = embed_tokens(images, w_patch, b_patch, pos_embed, ln1_gain, ln1_bias)
        w_qkv_t = jnp.transpose(w_qkv, (1, 2, 3, 0)).reshape(3 * dim, dim)
        o_t = attend_layer(normed, w_qkv_t, b_qkv, n_dev, num_heads, head_dim)
        num_images, band = normed.shape[:2]
        out = mlp_layer(o_t.reshape(num_images, dim, band), x_zero.reshape(num_images * band, dim), w_out.reshape(dim, dim),
                        b_out, ln2_gain, ln2_bias, w_fc1.T, b_fc1, w_fc2, b_fc2)
        return out.reshape(num_images, band, dim)

    in_specs = (P('dp', 'sp', None, None), P(), P(), P('sp', None), P(), P(), P(), P(), P(), P(), P(), P(), P(), P(), P(), P())
    return jax.shard_map(device_step, mesh=mesh, in_specs=in_specs, out_specs=P('dp', 'sp', None), check_vma=False)
```

```python
import functools
import math
import jax
import jax.numpy as jnp
import numpy as np
from jax import lax
from jax.experimental import pallas as pl
from jax.experimental.pallas import tpu as pltpu
from jax.sharding import PartitionSpec as P

LN_EPS = 1e-6
MESH = pl.DeviceIdType.MESH
F32 = jnp.float32
BF16 = jnp.bfloat16


def layer_norm(x_in, ln_gain, ln_bias):
    row_mean = jnp.mean(x_in, axis=-1, keepdims=True)
    centered = x_in - row_mean
    variance = jnp.mean(centered * centered, axis=-1, keepdims=True)
    return centered * lax.rsqrt(variance + LN_EPS) * ln_gain + ln_bias


def front_kernel(dims, img_hbm, wp_hbm, wq_hbm, pos_hbm, sel_ref, bp_ref, g1_ref, c1_ref, bq_ref, x_out, o_out,
                 img, wp, pos, w_f, w_s, perm_s, y_own, y_b, y_a, w_b, w_a, q_b, k_b, v_b, q_a, k_a, v_a,
                 s_buf, m_buf, p_buf, l_buf, o_b, o_a,
                 i_sem, p_sem, w_sem, y_send, y_recv, f_send, f_recv, o_send, o_recv):
    patch, n_dev, scale = dims
    n_chip = n_dev // 2
    n_img, chan, height, width = img.shape
    dim = y_own.shape[2]
    hd = v_a.shape[1]
    me = lax.axis_index('sp')
    chip = me // 2
    core = lax.rem(me, 2)
    sib = chip * 2 + (1 - core)
    heads = (w_b.shape[1] // hd, w_a.shape[1] // hd)
    head0 = ((lax.rem(chip, 2) * 2 + core) * heads[0], core * heads[1])
    y_units, w_units, o_units = (y_b, y_a), (w_b, w_a), (o_b, o_a)
    qkv_units = ((q_b, k_b, v_b), (q_a, k_a, v_a))

    def offset(b):
        return 2 - b + 3 * (b // 2) - 2 * (b // 3)

    def back(b):
        return (2 * b) % 3 + 3 * (b // 3)

    def owner_of(b):
        return lax.rem(chip + offset(b), n_chip)

    def image_of(owner, u):
        return (owner // 2) * 3 + (1 if u == 0 else 2 * lax.rem(owner, 2))

    order = [(1, 0), (1, 1), (1, 2), (1, 3), (0, 0), (0, 3)]
    wp_copy = pltpu.make_async_copy(wp_hbm, wp, p_sem.at[0])
    pos_copy = pltpu.make_async_copy(pos_hbm, pos, p_sem.at[1])
    wp_copy.start()
    img_copies = []
    for n, (u, b) in enumerate(order):
        c = pltpu.make_async_copy(img_hbm.at[image_of(owner_of(b), u)], img.at[n], i_sem.at[n])
        c.start()
        img_copies.append(c)
        if n == 0:
            pos_copy.start()
    w_copies = {}
    for u in (1, 0):
        for t in range(3):
            rows = heads[u] * hd
            c = pltpu.make_async_copy(
                wq_hbm.at[pl.ds(pl.multiple_of(t * dim + head0[u] * hd, 8), rows)], w_units[u].at[t], w_sem.at[u, t])
            c.start()
            w_copies[u, t] = c

    barrier = pltpu.get_barrier_semaphore()
    for j in range(1, n_dev):
        pl.semaphore_signal(barrier, inc=1, device_id={'sp': lax.rem(me + j, n_dev)}, device_id_type=MESH)

    cols = width // patch
    grid_rows = height // patch
    slab = sel_ref.shape[0] // grid_rows
    lanes = 128
    per_tile = lanes // cols
    out_col = lax.broadcasted_iota(jnp.int32, (1, width), 1)
    source = lax.rem(out_col, cols) * patch + out_col // cols
    perm_s[...] = jnp.where(lax.broadcasted_iota(jnp.int32, (width, width), 0) == source, 1.0, 0.0).astype(BF16)
    wp_copy.wait()

    def weights(n, carry):
        tile = pl.ds(pl.multiple_of(n * lanes, lanes), lanes)
        for q in range(patch):
            w_f[n, q * slab + slab - 8:(q + 1) * slab] = jnp.zeros((8, lanes), F32)
        for p in range(patch):
            for c in range(chan):
                w_f[n, pl.ds(c * patch + p, patch, stride=slab), :] = wp[p, c, :, tile].astype(F32)
        w_s[:, tile] = w_f[n].astype(BF16)
        return carry

    lax.fori_loop(0, w_f.shape[0], weights, 0)
    pos_copy.wait()
    lane_group = lax.broadcasted_iota(jnp.int32, (slab, lanes), 1) // cols

    def embed(n):
        u, b = order[n]
        img_copies[n].wait()
        pixels = img[n].reshape(chan * height, width).astype(BF16)
        rows = jnp.dot(sel_ref[...], pixels, preferred_element_type=F32).astype(BF16)
        z = jnp.dot(rows, perm_s[...], preferred_element_type=F32)
        z = jnp.concatenate([z, jnp.zeros((z.shape[0], -width % lanes), F32)], axis=1)
        blocks = []
        for q in range(patch):
            tile, off = q // per_tile, q % per_tile
            block = jnp.zeros((slab, lanes), F32)
            for y in range(grid_rows):
                part = z[y * slab:(y + 1) * slab, tile * lanes:(tile + 1) * lanes]
                shift = (y - off) % per_tile * cols
                if shift:
                    part = pltpu.roll(part, shift, 1)
                block = jnp.where(lane_group == y, part, block)
            blocks.append(block.astype(BF16))
        x_t = jnp.concatenate(blocks, axis=0)
        x0 = lax.dot_general(x_t, w_s[...], (((0,), (0,)), ((), ())), preferred_element_type=F32)
        x0 = (x0 + bp_ref[...].reshape(1, dim) + pos[...].astype(F32)).astype(BF16)
        i = image_of(owner_of(b), u)
        x_out[i] = x0
        y_own[i] = layer_norm(x0.astype(F32), g1_ref[...].reshape(1, dim), c1_ref[...].reshape(1, dim)).astype(BF16)

    def y_copy(u, b):
        return pltpu.make_async_remote_copy(
            y_own.at[image_of(owner_of(b), u)], y_units[u].at[back(b), core], y_send.at[u, b], y_recv.at[u, back(b)],
            device_id={'sp': owner_of(b) * 2 + core}, device_id_type=MESH)

    def own_copy(u):
        return pltpu.make_async_remote_copy(
            y_own.at[image_of(chip, u)], y_units[u].at[3, core], f_send.at[u, 3], f_recv.at[u, 3],
            device_id={'sp': sib}, device_id_type=MESH)

    def forward(u, b):
        return pltpu.make_async_remote_copy(
            y_units[u].at[b, core], y_units[u].at[b, core], f_send.at[u, b], f_recv.at[u, b],
            device_id={'sp': sib}, device_id_type=MESH)

    def send_y(n):
        u, b = order[n]
        if n < 3:
            y_copy(u, b).start()
        elif n == 3:
            own_copy(1).start()
        elif n == 4:
            y_copy(0, 0).start()
        else:
            y_copy(0, 1).start()
            y_copy(0, 2).start()
            own_copy(0).start()
        if b == 3:
            y_units[u][3, core] = y_own[image_of(chip, u)]

    embed(0)
    pl.semaphore_wait(barrier, n_dev - 1)
    for n in range(1, n_img):
        embed(n)
        send_y(n - 1)

    def project(u, b):
        y_chunk = y_units[u][b].reshape(-1, dim)
        width_b = y_chunk.shape[0]
        step = 4
        for t in range(3):
            for g in range(0, heads[u], step):
                prod = lax.dot_general(w_units[u][t, g * hd:(g + step) * hd], y_chunk, (((1,), (1,)), ((), ())),
                                       preferred_element_type=F32)
                bias = bq_ref[t, pl.ds(head0[u] + g, step)].T
                for h in range(step):
                    val = prod[h * hd:(h + 1) * hd] + bias[:, h:h + 1]
                    if t == 1:
                        qkv_units[u][t][g + h, width_b * b:width_b * (b + 1), :] = val.T.astype(BF16)
                    else:
                        qkv_units[u][t][g + h, :, width_b * b:width_b * (b + 1)] = val.astype(BF16)

    blk_len = s_buf.shape[2]

    def attend(u):
        q_u, k_u, v_u = qkv_units[u]
        o_u = o_units[u]
        n_head = heads[u]
        n_item = n_head * n_chip

        def scores(item, slot):
            h = lax.rem(item, n_head)
            blk = pl.ds(pl.multiple_of(item // n_head * blk_len, blk_len), blk_len)
            sc = jnp.dot(k_u[h], q_u[h, :, blk], preferred_element_type=F32)
            s_buf[slot] = sc
            m_buf[slot] = jnp.broadcast_to(jnp.max(sc, axis=0, keepdims=True), (8, blk_len))

        def weigh(slot):
            e = jnp.exp2((s_buf[slot] - m_buf[slot, :1]) * scale)
            l_buf[slot] = jnp.broadcast_to(jnp.sum(e, axis=0, keepdims=True), (8, blk_len))
            p_buf[slot] = e.astype(BF16)

        def mix(item, slot):
            h = lax.rem(item, n_head)
            b = item // n_head
            o = jnp.dot(v_u[h], p_buf[slot], preferred_element_type=F32) * (1.0 / l_buf[slot, :1])
            o = o.astype(BF16)
            o_u[b, 0, h] = o[:, :blk_len // 2]
            o_u[b, 1, h] = o[:, blk_len // 2:]

        scores(jnp.int32(0), 0)
        weigh(0)
        scores(jnp.int32(1), 1)

        def body(i, carry):
            scores(2 * i + 2, 0)
            weigh(1)
            mix(2 * i, 0)
            scores(2 * i + 3, 1)
            weigh(0)
            mix(2 * i + 1, 1)

            @pl.when((lax.rem(2 * i, n_head) == 0) & (i > 0))
            def _():
                send_o(u, (2 * i) // n_head - 1)
            return carry

        lax.fori_loop(0, n_item // 2 - 1, body, 0)
        weigh(1)
        mix(jnp.int32(n_item - 2), 0)
        mix(jnp.int32(n_item - 1), 1)

    def o_dst(owner, u, own_core):
        first = (lax.rem(owner, 2) * 2 + own_core) * heads[0] if u == 0 else own_core * heads[1]
        return o_out.at[image_of(owner, u), pl.ds(first, heads[u])]

    def o_copy(u, b, c2):
        dst_core = core if c2 == 0 else 1 - core
        return pltpu.make_async_remote_copy(
            o_units[u].at[b, dst_core], o_dst(chip, u, core), o_send.at[u, b, c2], o_recv.at[u, back(b), c2],
            device_id={'sp': owner_of(b) * 2 + dst_core}, device_id_type=MESH)

    def o_local(u):
        return pltpu.make_async_copy(o_units[u].at[3, core], o_dst(chip, u, core), o_recv.at[u, 3, 0])

    def send_o(u, b):
        if isinstance(b, int) and b == 3:
            o_copy(u, 3, 1).start()
            o_local(u).start()
        else:
            o_copy(u, b, 0).start()
            o_copy(u, b, 1).start()

    def gather(u, b):
        if b < 3:
            y_copy(u, back(b)).wait_recv()
            forward(u, b).start()
            pltpu.make_async_remote_copy(
                y_units[u].at[b, 1 - core], y_units[u].at[b, 1 - core], f_send.at[u, b], f_recv.at[u, b],
                device_id={'sp': sib}, device_id_type=MESH).wait_recv()
        else:
            own_copy(u).wait_recv()

    for t in range(3):
        w_copies[1, t].wait()
    gather(1, 3)
    project(1, 3)
    send_y(n_img - 1)
    for t in range(3):
        w_copies[0, t].wait()
    gather(0, 3)
    project(0, 3)
    for b in (1, 2, 0):
        gather(1, b)
        project(1, b)
    attend(1)
    send_o(1, 3)
    for b in (1, 2, 0):
        gather(0, b)
        project(0, b)
    attend(0)
    send_o(0, 3)

    for u in range(2):
        own_copy(u).wait_send()
        for b in range(3):
            y_copy(u, b).wait_send()
            forward(u, b).wait_send()
            for c2 in range(2):
                o_copy(u, b, c2).wait_send()
        o_copy(u, 3, 1).wait_send()
        o_local(u).wait()
    for u in range(2):
        for b in range(n_chip):
            for c2 in range(2):
                if b == 3 and c2 == 0:
                    continue
                src_core = core if c2 == 0 else 1 - core
                pltpu.make_async_remote_copy(
                    o_units[u].at[b, 0], o_dst(owner_of(b), u, src_core), o_send.at[u, b, c2], o_recv.at[u, b, c2],
                    device_id={'sp': sib}, device_id_type=MESH).wait_recv()


def front_layer(images, w_patch, b_patch, pos_embed, ln1_gain, ln1_bias, w_qkv, b_qkv, n_dev):
    n_img, height, width, chan = images.shape
    patch, dim = w_patch.shape[0], w_patch.shape[3]
    n_head, hd = w_qkv.shape[2:]
    n_chip = n_dev // 2
    grid_rows = height // patch
    band = pos_embed.shape[0]
    slab = -(-chan * patch // 16) * 16
    select = np.zeros((grid_rows * slab, chan * height), np.float32)
    for y in range(grid_rows):
        for c in range(chan):
            for p in range(patch):
                select[y * slab + c * patch + p, c * height + y * patch + p] = 1.0
    depth = patch * slab
    keys = band * n_dev
    scale = hd ** -0.5 * math.log2(math.e)
    heads_b, heads_a = n_head // 4, n_head // 2
    blk = 2 * band

    def unit(heads):
        return [pltpu.VMEM((heads, hd, keys), BF16), pltpu.VMEM((heads, keys, hd), BF16), pltpu.VMEM((heads, hd, keys), BF16)]

    vmem = pl.BlockSpec(memory_space=pltpu.VMEM)
    hbm = pl.BlockSpec(memory_space=pl.ANY)
    dma = pltpu.SemaphoreType.DMA
    return pl.pallas_call(
        functools.partial(front_kernel, (patch, n_dev, scale)),
        out_shape=[jax.ShapeDtypeStruct((n_img, band, dim), BF16), jax.ShapeDtypeStruct((n_img, n_head, hd, band), BF16)],
        in_specs=[hbm] * 4 + [vmem] * 5,
        out_specs=[vmem, hbm],
        scratch_shapes=[
            pltpu.VMEM((n_img, chan, height, width), F32), pltpu.VMEM((patch, chan, patch, dim), BF16),
            pltpu.VMEM((band, dim), BF16),
            pltpu.VMEM((dim // 128, depth, 128), F32), pltpu.VMEM((depth, dim), BF16), pltpu.VMEM((width, width), BF16),
            pltpu.VMEM((n_img, band, dim), BF16),
            pltpu.VMEM((n_chip, 2, band, dim), BF16), pltpu.VMEM((n_chip, 2, band, dim), BF16),
            pltpu.VMEM((3, heads_b * hd, dim), BF16), pltpu.VMEM((3, heads_a * hd, dim), BF16),
            *unit(heads_b), *unit(heads_a),
            pltpu.VMEM((2, keys, blk), F32), pltpu.VMEM((2, 8, blk), F32),
            pltpu.VMEM((2, keys, blk), BF16), pltpu.VMEM((2, 8, blk), F32),
            pltpu.VMEM((n_chip, 2, heads_b, hd, band), BF16), pltpu.VMEM((n_chip, 2, heads_a, hd, band), BF16),
            dma((n_img,)), dma((2,)), dma((2, 3)), dma((2, n_chip)), dma((2, n_chip)), dma((2, n_chip)), dma((2, n_chip)),
            dma((2, n_chip, 2)), dma((2, n_chip, 2)),
        ],
        compiler_params=pltpu.CompilerParams(collective_id=0, has_side_effects=True, vmem_limit_bytes=60 * 2**20),
        name='front',
    )(jnp.transpose(images, (0, 3, 1, 2)), jnp.transpose(w_patch, (0, 2, 1, 3)),
      jnp.transpose(w_qkv, (1, 2, 3, 0)).reshape(3 * dim, dim), pos_embed, jnp.asarray(select, BF16),
      b_patch, ln1_gain, ln1_bias, b_qkv)


def mlp_kernel(chunk, tail, o_ref, x_ref, wo_ref, bo_ref, g2_ref, c2_ref, b1_ref, b2_ref, w1_hbm, w2_hbm, out_ref,
               w1, w2, acc, y2, hid, sem1, sem2):
    n_full = (w1.shape[0] - tail) // chunk

    def w_copy(i, size):
        rows = pl.ds(i * chunk, size) if isinstance(i, int) else pl.ds(pl.multiple_of(i * chunk, chunk), size)
        return (pltpu.make_async_copy(w1_hbm.at[rows], w1.at[rows], sem1.at[i]),
                pltpu.make_async_copy(w2_hbm.at[rows], w2.at[rows], sem2.at[i]))

    for i in range(n_full + 1):
        for c in w_copy(i, chunk if i < n_full else tail):
            c.start()
    n_img, dim, band = o_ref.shape

    def proj(i, carry):
        rows = pl.ds(pl.multiple_of(i * band, band), band)
        r = lax.dot_general(o_ref[i], wo_ref[...], (((0,), (0,)), ((), ())), preferred_element_type=F32)
        r = x_ref[rows].astype(F32) + r + bo_ref[...].reshape(1, dim)
        acc[rows] = r + b2_ref[...].reshape(1, dim)
        y2[rows] = layer_norm(r, g2_ref[...].reshape(1, dim), c2_ref[...].reshape(1, dim)).astype(BF16)
        return carry

    lax.fori_loop(0, n_img, proj, 0)

    def first(i, size, slot):
        rows = pl.ds(i * chunk, size) if isinstance(i, int) else pl.ds(pl.multiple_of(i * chunk, chunk), size)
        pre = lax.dot_general(y2[...], w1[rows], (((1,), (1,)), ((), ())), preferred_element_type=F32)
        pre = pre + b1_ref[:, rows]
        hid[slot, :, :size] = jax.nn.gelu(pre, approximate=True).astype(BF16)

    def second(i, size, slot):
        rows = pl.ds(i * chunk, size) if isinstance(i, int) else pl.ds(pl.multiple_of(i * chunk, chunk), size)
        acc[...] += jnp.dot(hid[slot, :, :size], w2[rows], preferred_element_type=F32)

    w_copy(0, chunk)[0].wait()
    first(0, chunk, 0)

    def body(i, carry):
        w_copy(i + 1, chunk)[0].wait()
        w_copy(i, chunk)[1].wait()
        first(i + 1, chunk, lax.rem(i + 1, 2))
        second(i, chunk, lax.rem(i, 2))
        return carry

    lax.fori_loop(0, n_full - 1, body, 0)
    w_copy(n_full, tail)[0].wait()
    w_copy(n_full - 1, chunk)[1].wait()
    first(n_full, tail, n_full % 2)
    second(n_full - 1, chunk, (n_full - 1) % 2)
    w_copy(n_full, tail)[1].wait()
    second(n_full, tail, n_full % 2)
    out_ref[...] = acc[...].astype(BF16)


def mlp_layer(o_t, x_zero, w_out, b_out, ln2_gain, ln2_bias, w_fc1_t, b_fc1, w_fc2, b_fc2):
    images, dim, band = o_t.shape
    ff = w_fc2.shape[0]
    rows = images * band
    chunk = 512
    tail = ff - (ff - 1) // chunk * chunk
    n_chunks = (ff - tail) // chunk + 1
    vmem = pl.BlockSpec(memory_space=pltpu.VMEM)
    hbm = pl.BlockSpec(memory_space=pl.ANY)
    flops = 2 * rows * dim * (dim + 2 * ff)
    return pl.pallas_call(
        functools.partial(mlp_kernel, chunk, tail),
        out_shape=jax.ShapeDtypeStruct((rows, dim), BF16),
        in_specs=[vmem] * 8 + [hbm, hbm],
        out_specs=vmem,
        scratch_shapes=[
            pltpu.VMEM((ff, dim), BF16), pltpu.VMEM((ff, dim), BF16), pltpu.VMEM((rows, dim), F32),
            pltpu.VMEM((rows, dim), BF16), pltpu.VMEM((2, rows, chunk), BF16),
            pltpu.SemaphoreType.DMA((n_chunks,)), pltpu.SemaphoreType.DMA((n_chunks,)),
        ],
        compiler_params=pltpu.CompilerParams(vmem_limit_bytes=56 * 2**20),
        cost_estimate=pl.CostEstimate(flops=flops, bytes_accessed=32 * 2**20, transcendentals=0),
        name='mlp',
    )(o_t, x_zero, w_out, b_out, ln2_gain, ln2_bias, b_fc1[None], b_fc2, w_fc1_t, w_fc2)


def solution(mesh):
    n_dev = mesh.shape['sp']

    def device_step(images, w_patch, b_patch, pos_embed, ln1_gain, ln1_bias, w_qkv, b_qkv, w_out, b_out, ln2_gain, ln2_bias, w_fc1, b_fc1, w_fc2, b_fc2):
        dim, _, num_heads, head_dim = w_qkv.shape
        x_zero, o_t = front_layer(images, w_patch, b_patch, pos_embed, ln1_gain, ln1_bias, w_qkv, b_qkv, n_dev)
        num_images, band = x_zero.shape[:2]
        out = mlp_layer(o_t.reshape(num_images, dim, band), x_zero.reshape(num_images * band, dim), w_out.reshape(dim, dim),
                        b_out, ln2_gain, ln2_bias, w_fc1.T, b_fc1, w_fc2, b_fc2)
        return out.reshape(num_images, band, dim)

    in_specs = (P('dp', 'sp', None, None), P(), P(), P('sp', None), P(), P(), P(), P(), P(), P(), P(), P(), P(), P(), P(), P())
    return jax.shard_map(device_step, mesh=mesh, in_specs=in_specs, out_specs=P('dp', 'sp', None), check_vma=False)
```
